32 devices in a mesh: fsdp: 8 (over z, x), rep: 4 (over y, core).
Axes of the slice: x: 2, y: 2, z: 4, core: 2. Of those that a mesh axis runs over, the one named last changes fastest.
Arguments:
- cross_base: bfloat16 [4096, 4096], P(('fsdp', 'rep')), may hold values from -6 to 6
- layer_in: bfloat16 [4096, 4096], P(('fsdp', 'rep')), may hold values from -6 to 6
- grad_out: bfloat16 [4096, 4096], P(('fsdp', 'rep')), may hold values from -6 to 6
- reduce_a: bfloat16 [4096, 256], P('fsdp'), may hold values from -0.09375 to 0.09375
- expand_a: bfloat16 [4096, 256], P('fsdp'), may hold values from -0.375 to 0.375
- reduce_b: bfloat16 [4096, 256], P('fsdp'), may hold values from -0.09375 to 0.09375
- expand_b: bfloat16 [4096, 256], P('fsdp'), may hold values from -0.375 to 0.375
Outputs:
- grad_layer_in: bfloat16 [4096, 4096], P(('fsdp', 'rep'))
- grad_base: bfloat16 [4096, 4096], P(('fsdp', 'rep'))
- grad_reduce_a: float32 [4096, 256], P('fsdp')
- grad_expand_a: float32 [4096, 256], P('fsdp')
- grad_reduce_b: float32 [4096, 256], P('fsdp')
- grad_expand_b: float32 [4096, 256], P('fsdp')
The draws below stay inside these ranges and needn't reach their ends.
All inputs are finite; a program needn't handle non-finite values.
Results may differ from the reference program's by a relative error of at most 0.015.
Values may be sent and summed in bfloat16 or wider, within the bound.
A program may use at most 128 MiB of HBM per device.

```python
import math
import jax
import jax.numpy as jnp
from jax import lax

D = 4096
RANK = 256
TOKENS = 4096


def with_spikes(array, own_key, source, target, parts, factor):
    owner, partner = [(jnp.arange(array.shape[position]) // (array.shape[position] // parts)).reshape([-1 if axis == position else 1 for axis in range(array.ndim)]) for position in (source, target)]
    chosen = jax.random.permutation(own_key, parts)[partner]
    strong = (owner == chosen) | (owner == (partner + parts // 2) % parts)
    return jnp.where(strong, factor * array, array)


def block_scale(key, extent, split, smallest, largest):
    factor_of, own = 1.0, jax.random.fold_in(key, 6)
    for dim, parts in split:
        heights = jnp.exp(jax.random.uniform(jax.random.fold_in(own, dim), (parts,), jnp.float32, smallest / len(split), largest / len(split)))
        factor_of = factor_of * jnp.repeat(heights, extent[dim] // parts).reshape([-1 if axis == dim else 1 for axis in range(len(extent))])
    return factor_of


def gaussian(stream_key, dims, scale, most, pieces=(), kind=jnp.bfloat16):
    level = block_scale(stream_key, dims, pieces, -0.22, 0.18) if pieces else 1.0
    drawn = jax.random.normal(stream_key, dims, jnp.float32) * scale * level
    return jnp.minimum(jnp.maximum(drawn, -most), most).astype(kind)


def gaussian_with(own_key, shape, width, reach, pieces, heavy, held_as=jnp.bfloat16):
    result = width * jax.random.normal(own_key, shape, jnp.float32)
    if pieces:
        result = result * block_scale(own_key, shape, pieces, -0.22, 0.18)
    return jnp.clip(with_spikes(result, jax.random.fold_in(own_key, 3), *heavy), -reach, reach).astype(held_as)


def setup_inputs(seed: int = 0) -> dict:
    splits = jax.random.split(jax.random.key(seed), 8)
    return {
        "cross_base": gaussian(splits[0], (TOKENS, D), 1.0, 6.0, ((0, 32),)),
        "layer_in": gaussian(splits[1], (TOKENS, D), 1.0, 6.0, ((0, 32),)),
        "grad_out": gaussian_with(splits[2], (TOKENS, D), 1.0, 6.0, ((0, 32),), (0, 1, 32, 2.75)),
        "reduce_a": gaussian(splits[3], (D, RANK), D ** -0.5, 0.09375, ((0, 8),)),
        "expand_a": gaussian(splits[4], (D, RANK), RANK ** -0.5, 0.375, ((0, 8),)),
        "reduce_b": gaussian(splits[5], (D, RANK), D ** -0.5, 0.09375, ((0, 8),)),
        "expand_b": gaussian(splits[6], (D, RANK), RANK ** -0.5, 0.375, ((0, 8),)),
    }


def contract_rows(left, right):
    return lax.dot_general(left, right, (((0,), (0,)), ((), ())), preferred_element_type=jnp.float32)

def contract_cols(left, right):
    return lax.dot_general(left, right, (((1,), (1,)), ((), ())), preferred_element_type=jnp.float32)

def project(inputs, reduce_full, expand_full):
    narrow = jnp.dot(inputs, reduce_full, preferred_element_type=jnp.float32).astype(jnp.bfloat16)
    return (narrow, contract_cols(narrow, expand_full))

def local_backward(grad_in, cross_base, reduce_full, expand_full):
    grad_wide = grad_in.astype(jnp.float32)
    masked = (grad_wide * cross_base.astype(jnp.float32)).astype(jnp.bfloat16)
    narrow_grad = jnp.dot(masked, expand_full, preferred_element_type=jnp.float32).astype(jnp.bfloat16)
    passed = grad_wide + contract_cols(narrow_grad, reduce_full)
    return (masked, narrow_grad, passed)

def reference(cross_base, layer_in, grad_out, reduce_a, expand_a, reduce_b, expand_b):
    factor = 1.0 / math.sqrt(TOKENS)
    base_wide = cross_base.astype(jnp.float32)
    narrow_a, cross_a = project(layer_in, reduce_a, expand_a)
    middle = (layer_in.astype(jnp.float32) + base_wide * cross_a).astype(jnp.bfloat16)
    narrow_b, cross_b = project(middle, reduce_b, expand_b)
    masked_b, narrow_grad_b, passed_b = local_backward(grad_out, cross_base, reduce_b, expand_b)
    grad_expand_b = contract_rows(masked_b, narrow_b) * factor
    grad_reduce_b = contract_rows(middle, narrow_grad_b) * factor
    grad_middle = passed_b.astype(jnp.bfloat16)
    masked_a, narrow_grad_a, passed_a = local_backward(grad_middle, cross_base, reduce_a, expand_a)
    grad_expand_a = contract_rows(masked_a, narrow_a) * factor
    grad_reduce_a = contract_rows(layer_in, narrow_grad_a) * factor
    grad_layer_in = passed_a.astype(jnp.bfloat16)
    grad_base = (grad_out.astype(jnp.float32) * cross_b + grad_middle.astype(jnp.float32) * cross_a).astype(jnp.bfloat16)
    return (grad_layer_in, grad_base, grad_reduce_a, grad_expand_a, grad_reduce_b, grad_expand_b)
```

```python
import functools
import math

import jax
import jax.numpy as jnp
from jax import lax
from jax.experimental import pallas as pl
from jax.experimental.pallas import tpu as pltpu
from jax.sharding import PartitionSpec as P

MESH = pl.DeviceIdType.MESH
F32 = jnp.float32
BF16 = jnp.bfloat16


def dot_nn(left, right):
    return lax.dot_general(left, right, (((1,), (0,)), ((), ())), preferred_element_type=F32)


def dot_nt(left, right):
    return lax.dot_general(left, right, (((1,), (1,)), ((), ())), preferred_element_type=F32)


def dot_tn(left, right):
    return lax.dot_general(left, right, (((0,), (0,)), ((), ())), preferred_element_type=F32)


def kernel(
    F,
    R,
    factor,
    base_in,
    lin_in,
    gout_in,
    ra,
    ea,
    rb,
    eb,
    gli_out,
    gbase_out,
    grads_out,
    base,
    gout,
    own,
    nar,
    peer_wide,
    peer_nar,
    full,
    cross_a,
    gmid,
    gli,
    gbase,
    part,
    grads,
    x1_send,
    x1_recv,
    z1_send,
    z1_recv,
    z2_send,
    z2_recv,
    x2_send,
    x2_recv,
    ybuf,
    load_sem,
    out_sem,
    ag_recv,
    ag_z,
    ag_x,
    ag_d,
    ag_drecv,
    pw_sem,
    pn_sem,
    x1_sem,
    z1_sem,
    z2_sem,
    x2_sem,
    y_ssem,
    y_rsem,
    g_sem,
):
    X = 2
    Z = F // X
    Y = R // 2
    rows = ra.shape[0]
    half = rows // 2
    D = base.shape[1]
    f = lax.axis_index("fsdp")
    r = lax.axis_index("rep")
    z, x = f // X, f % X
    y, c = r // 2, r % 2
    xo = 1 - x
    zp, zm = (z + 1) % Z, (z + Z - 1) % Z

    def dev(ff, rr):
        return {"fsdp": ff, "rep": rr}

    up, down = dev(zp * X + x, r), dev(zm * X + x, r)
    across = dev(z * X + xo, r)
    mate = dev(f, y * 2 + 1 - c)

    def ymate(i):
        return dev(f, ((y + i) % Y) * 2 + c)

    loads = []
    for i, (src, dst) in enumerate(
        (
            (ra, full.at[0, pl.ds(pl.multiple_of(f * rows, rows), rows), :]),
            (ea, full.at[1, pl.ds(pl.multiple_of(f * rows, rows), rows), :]),
            (rb, full.at[2, pl.ds(pl.multiple_of(f * rows, rows), rows), :]),
            (eb, full.at[3, pl.ds(pl.multiple_of(f * rows, rows), rows), :]),
            (base_in, base),
            (gout_in, gout),
            (lin_in, own.at[0, 0]),
        )
    ):
        copy = pltpu.make_async_copy(src, dst, load_sem.at[i])
        copy.start()
        loads.append(copy)

    barrier = pltpu.get_barrier_semaphore()
    friends = [up, down, across, mate] + [ymate(i) for i in range(1, Y)]
    for friend in friends:
        pl.semaphore_signal(barrier, inc=1, device_id=friend, device_id_type=MESH)
    pl.semaphore_wait(barrier, len(friends))
    for copy in loads[:4]:
        copy.wait()

    def piece(w, zz, xx, h):
        start = ((zz + 2 * Z) % Z * X + xx) * rows + h * half
        return full.at[w, pl.ds(pl.multiple_of(start, half), half), :]

    def slot(zz, xx):
        return (zz + 2 * Z) % Z * X + xx

    sent = []

    def send(ref, ssem, rsem, target):
        copy = pltpu.make_async_remote_copy(
            src_ref=ref, dst_ref=ref, send_sem=ssem, recv_sem=rsem,
            device_id=target, device_id_type=MESH,
        )
        copy.start()
        sent.append(copy)

    def zsend(k, zz, xx, h):
        o = slot(zz, xx)
        send(piece(2 * c + k, zz, xx, h), ag_z.at[k, o, h], ag_recv.at[k, o, h], down if h else up)

    def xsend(k, zz, xx, h):
        o = slot(zz, xx)
        send(piece(2 * c + k, zz, xx, h), ag_x.at[k, o, h], ag_recv.at[k, o, h], across)

    def dsend(k, zz, xx, h):
        o = slot(zz, xx)
        send(piece(2 * c + k, zz, xx, h), ag_d.at[k, o, h], ag_drecv.at[k, o, h], mate)

    def arrive(k, zz, xx, h):
        o = slot(zz, xx)
        ref = piece(2 * c + k, zz, xx, h)
        pltpu.make_async_remote_copy(
            src_ref=ref, dst_ref=ref, send_sem=ag_z.at[k, o, h], recv_sem=ag_recv.at[k, o, h],
            device_id=up, device_id_type=MESH,
        ).wait_recv()

    for h in range(2):
        zsend(1, z, x, h)
        xsend(0, z, x, h)
    for h in range(2):
        zsend(0, z, x, h)
        xsend(1, z, x, h)

    for copy in loads[4:]:
        copy.wait()
    tile = min(512, D)

    @pl.loop(0, D // tile)
    def _(t):
        cols = pl.ds(pl.multiple_of(t * tile, tile), tile)
        own[1, 1, :, cols] = (gout[:, cols].astype(F32) * base[:, cols].astype(F32)).astype(BF16)

    for s in range(1, Z + 1):
        for h in range(2):
            sign = 1 if h else -1
            if s < Z:
                zz = z + sign * s
                arrive(1, zz, x, h)
                if s < Z - 1:
                    zsend(1, zz, x, h)
                xsend(1, zz, x, h)
                dsend(1, zz, x, h)
            zo = z + sign * (s - 1)
            arrive(0, zo, xo, h)
            if s < Z:
                zsend(0, zo, xo, h)
            dsend(0, zo, xo, h)
            if s < Z:
                zz = z + sign * s
                arrive(0, zz, x, h)
                if s < Z - 1:
                    zsend(0, zz, x, h)
                dsend(0, zz, x, h)
        for h in range(2):
            sign = 1 if h else -1
            zo = z + sign * (s - 1)
            arrive(1, zo, xo, h)
            dsend(1, zo, xo, h)
    for k in range(2):
        for s in range(Z):
            for xx in (x, xo):
                if s == 0 and xx is x:
                    continue
                for h in range(2):
                    zz = z + (s if h else -s)
                    o = slot(zz, xx)
                    ref = piece(2 * (1 - c) + k, zz, xx, h)
                    pltpu.make_async_remote_copy(
                        src_ref=ref, dst_ref=ref, send_sem=ag_d.at[k, o, h],
                        recv_sem=ag_drecv.at[k, o, h], device_id=mate, device_id_type=MESH,
                    ).wait_recv()
    for copy in sent:
        copy.wait_send()

    nar[0, 1] = dot_nn(own[0, 0], full[0]).astype(BF16)
    nar[1, 0] = dot_nn(own[1, 1], full[3]).astype(BF16)

    @pl.loop(0, D // tile)
    def _(t):
        cols = pl.ds(pl.multiple_of(t * tile, tile), tile)
        wide = base[:, cols].astype(F32)
        crossed = dot_nt(nar[0, 1], full[1, cols, :])
        cross_a[:, cols] = crossed
        own[1, 0, :, cols] = (own[0, 0, :, cols].astype(F32) + wide * crossed).astype(BF16)
        passed = (gout[:, cols].astype(F32) + dot_nt(nar[1, 0], full[2, cols, :])).astype(BF16)
        gmid[:, cols] = passed
        own[0, 1, :, cols] = (passed.astype(F32) * wide).astype(BF16)

    nar[1, 1] = dot_nn(own[1, 0], full[2]).astype(BF16)
    nar[0, 0] = dot_nn(own[0, 1], full[1]).astype(BF16)

    swaps = []
    for k in range(2):
        for src, dst, sem in ((own, peer_wide, pw_sem), (nar, peer_nar, pn_sem)):
            copy = pltpu.make_async_remote_copy(
                src_ref=src.at[1 - c, k], dst_ref=dst.at[k], send_sem=sem.at[0, k],
                recv_sem=sem.at[1, k], device_id=mate, device_id_type=MESH,
            )
            copy.start()
            swaps.append(copy)

    def push(src, dst, sems, target):
        copy = pltpu.make_async_remote_copy(
            src_ref=src, dst_ref=dst, send_sem=sems[0], recv_sem=sems[1],
            device_id=target, device_id_type=MESH,
        )
        copy.start()
        return copy

    for copy in swaps:
        copy.wait()

    @pl.loop(0, D // tile)
    def _(t):
        cols = pl.ds(pl.multiple_of(t * tile, tile), tile)
        for k in range(2):
            part[k, cols, :] = dot_tn(own[c, k, :, cols], nar[c, k]) + dot_tn(
                peer_wide[k, :, cols], peer_nar[k]
            )

    def mine(k, zz, xx, h=None):
        start = slot(zz, xx) * rows
        if h is None:
            return part[k, pl.ds(pl.multiple_of(start, rows), rows), :]
        return part[k, pl.ds(pl.multiple_of(start + h * half, half), half), :]

    hx1, hz1, hz2 = {}, {}, {}

    def send_z2(s):
        for h in range(2):
            zz = z + (1 + s) * (1 if h else -1)
            for i, xx in enumerate((x, xo)):
                value = mine(1, zz, xx, h)
                if s > 0:
                    hz2[s - 1, h, i].wait_recv()
                    value = value + z2_recv[s - 1, h, i].astype(F32)
                z2_send[s, h, i] = value.astype(BF16)
                hz2[s, h, i] = push(
                    z2_send.at[s, h, i], z2_recv.at[s, h, i],
                    (z2_sem.at[0, s, h, i], z2_sem.at[1, s, h, i]), down if h else up,
                )

    def send_z1(s):
        for h in range(2):
            zz = z + (1 + s) * (1 if h else -1)
            value = mine(0, zz, x, h)
            value = value + x1_recv[(zz + 2 * Z) % Z, pl.ds(h * half, half), :].astype(F32)
            if s > 0:
                hz1[s - 1, h].wait_recv()
                value = value + z1_recv[s - 1, h].astype(F32)
            z1_send[s, h] = value.astype(BF16)
            hz1[s, h] = push(
                z1_send.at[s, h], z1_recv.at[s, h],
                (z1_sem.at[0, s, h], z1_sem.at[1, s, h]), down if h else up,
            )

    send_z2(0)
    order = []
    for d in range(1, Z):
        order.append(d // 2 + 1 if d % 2 else -(d // 2))
    order.append(0)
    for i, d in enumerate(order):
        zz = (z + d + 2 * Z) % Z
        x1_send[zz] = mine(0, zz, xo).astype(BF16)
        hx1[i] = push(
            x1_send.at[zz], x1_recv.at[zz], (x1_sem.at[0, zz], x1_sem.at[1, zz]), across
        )

    @pl.loop(0, D // tile)
    def _(t):
        cols = pl.ds(pl.multiple_of(t * tile, tile), tile)
        held = gmid[:, cols].astype(F32)
        crossed = dot_nt(nar[1, 1], full[3, cols, :])
        gbase[:, cols] = (gout[:, cols].astype(F32) * crossed + held * cross_a[:, cols]).astype(BF16)
        gli[:, cols] = (held + dot_nt(nar[0, 0], full[0, cols, :])).astype(BF16)

    outs = []
    for i, (src, dst) in enumerate(((gli, gli_out), (gbase, gbase_out))):
        copy = pltpu.make_async_copy(src, dst, out_sem.at[i])
        copy.start()
        outs.append(copy)

    for s in range(1, Z - 1):
        send_z2(s)
    for h in range(2):
        for i in range(2):
            hz2[Z - 2, h, i].wait_recv()
    for h in range(2):
        x2_send[pl.ds(h * half, half), :] = (
            mine(1, z, xo, h) + z2_recv[Z - 2, h, 1].astype(F32)
        ).astype(BF16)
    hx2 = push(x2_send, x2_recv, (x2_sem.at[0], x2_sem.at[1]), across)
    for i in range(Z):
        hx1[i].wait_recv()
    for s in range(Z - 1):
        send_z1(s)

    hy = []

    def send_y(k):
        for i in range(1, Y):
            hy.append(
                push(ybuf.at[k, y], ybuf.at[k, y], (y_ssem.at[k, i], y_rsem.at[k, i]), ymate(i))
            )

    hx2.wait_recv()
    for h in range(2):
        ybuf[1, y, pl.ds(h * half, half), :] = (
            mine(1, z, x, h)
            + z2_recv[Z - 2, h, 0].astype(F32)
            + x2_recv[pl.ds(h * half, half), :].astype(F32)
        ).astype(BF16)
    send_y(1)
    for h in range(2):
        hz1[Z - 2, h].wait_recv()
        ybuf[0, y, pl.ds(h * half, half), :] = (
            mine(0, z, x, h)
            + x1_recv[z, pl.ds(h * half, half), :].astype(F32)
            + z1_recv[Z - 2, h].astype(F32)
        ).astype(BF16)
    send_y(0)
    hg = []
    for j, k in enumerate((1, 0)):
        for i in range(Y - 1):
            from_y = (y + Y - (i + 1)) % Y
            pltpu.make_async_remote_copy(
                src_ref=ybuf.at[k, from_y], dst_ref=ybuf.at[k, from_y],
                send_sem=y_ssem.at[k, i + 1], recv_sem=y_rsem.at[k, i + 1],
                device_id=ymate(i + 1), device_id_type=MESH,
            ).wait_recv()
        total = ybuf[k, 0].astype(F32)
        for i in range(1, Y):
            total = total + ybuf[k, i].astype(F32)
        grads[2 * c + k] = total * factor
        hg.append(
            push(grads.at[2 * c + k], grads.at[2 * c + k], (g_sem.at[0, k], g_sem.at[1, k]), mate)
        )
    for k in range(2):
        w = 2 * (1 - c) + k
        pltpu.make_async_remote_copy(
            src_ref=grads.at[w], dst_ref=grads.at[w], send_sem=g_sem.at[0, k],
            recv_sem=g_sem.at[1, k], device_id=mate, device_id_type=MESH,
        ).wait_recv()
    last = pltpu.make_async_copy(grads, grads_out, out_sem.at[2])
    last.start()
    for copy in list(hx1.values()) + list(hz1.values()) + list(hz2.values()) + [hx2] + hy + hg:
        copy.wait_send()
    for copy in outs + [last]:
        copy.wait()


def solution(mesh):
    F, R = mesh.shape["fsdp"], mesh.shape["rep"]
    X = 2
    Z, Y = F // X, R // 2

    def on_device(base, lin, gout, ra, ea, rb, eb):
        T, D = base.shape
        rows, K = ra.shape
        half = rows // 2
        factor = 1.0 / math.sqrt(T * F * R)
        dma = pltpu.SemaphoreType.DMA
        vm = pltpu.VMEM
        any_spec = pl.BlockSpec(memory_space=pl.ANY)
        gli, gbase, grads = pl.pallas_call(
            functools.partial(kernel, F, R, factor),
            out_shape=(
                jax.ShapeDtypeStruct((T, D), BF16),
                jax.ShapeDtypeStruct((T, D), BF16),
                jax.ShapeDtypeStruct((4, rows, K), F32),
            ),
            in_specs=[any_spec] * 7,
            out_specs=[any_spec] * 3,
            scratch_shapes=[
                vm((T, D), BF16),
                vm((T, D), BF16),
                vm((2, 2, T, D), BF16),
                vm((2, 2, T, K), BF16),
                vm((2, T, D), BF16),
                vm((2, T, K), BF16),
                vm((4, D, K), BF16),
                vm((T, D), F32),
                vm((T, D), BF16),
                vm((T, D), BF16),
                vm((T, D), BF16),
                vm((2, D, K), F32),
                vm((4, rows, K), F32),
                vm((Z, rows, K), BF16),
                vm((Z, rows, K), BF16),
                vm((Z - 1, 2, half, K), BF16),
                vm((Z - 1, 2, half, K), BF16),
                vm((Z - 1, 2, 2, half, K), BF16),
                vm((Z - 1, 2, 2, half, K), BF16),
                vm((rows, K), BF16),
                vm((rows, K), BF16),
                vm((2, Y, rows, K), BF16),
                dma((7,)),
                dma((3,)),
                dma((2, F, 2)),
                dma((2, F, 2)),
                dma((2, F, 2)),
                dma((2, F, 2)),
                dma((2, F, 2)),
                dma((2, 2)),
                dma((2, 2)),
                dma((2, Z)),
                dma((2, Z - 1, 2)),
                dma((2, Z - 1, 2, 2)),
                dma((2,)),
                dma((2, Y)),
                dma((2, Y)),
                dma((2, 2)),
            ],
            compiler_params=pltpu.CompilerParams(
                collective_id=1, has_side_effects=True, vmem_limit_bytes=60 * 1024 * 1024
            ),
        )(base, lin, gout, ra, ea, rb, eb)
        return gli, gbase, grads[0], grads[1], grads[2], grads[3]

    both = P(("fsdp", "rep"), None)
    one = P("fsdp", None)
    return jax.shard_map(
        on_device,
        mesh=mesh,
        in_specs=(both, both, both, one, one, one, one),
        out_specs=(both, both, one, one, one, one),
        check_vma=False,
    )
```

```python
import functools
import math

import jax
import jax.numpy as jnp
from jax import lax
from jax.experimental import pallas as pl
from jax.experimental.pallas import tpu as pltpu
from jax.sharding import PartitionSpec as P

MESH = pl.DeviceIdType.MESH
F32 = jnp.float32
BF16 = jnp.bfloat16


def dot_nn(left, right):
    return lax.dot_general(left, right, (((1,), (0,)), ((), ())), preferred_element_type=F32)


def dot_nt(left, right):
    return lax.dot_general(left, right, (((1,), (1,)), ((), ())), preferred_element_type=F32)


def dot_tn(left, right):
    return lax.dot_general(left, right, (((0,), (0,)), ((), ())), preferred_element_type=F32)


def kernel(
    F,
    R,
    factor,
    base_in,
    lin_in,
    gout_in,
    ra,
    ea,
    rb,
    eb,
    gli_out,
    gbase_out,
    grads_out,
    base,
    gout,
    own,
    nar,
    peer_wide,
    peer_nar,
    full,
    cross_a,
    gmid,
    gli,
    gbase,
    part,
    grads,
    y1_send,
    y1_recv,
    x1_send,
    x1_recv,
    x2_send,
    x2_recv,
    y2_send,
    y2_recv,
    z_send,
    z_recv,
    last_sum,
    fin,
    load_sem,
    out_sem,
    ag_recv,
    ag_z,
    ag_x,
    ag_y,
    ag_d,
    ag_drecv,
    pw_sem,
    pn_sem,
    y1_sem,
    x1_sem,
    x2_sem,
    y2_sem,
    zs_sem,
    zr_sem,
    y_ssem,
    y_rsem,
    g_sem,
):
    X = 2
    Z = F // X
    rows = ra.shape[0]
    half = rows // 2
    D = base.shape[1]
    f = lax.axis_index("fsdp")
    r = lax.axis_index("rep")
    z, x = f // X, f % X
    y, c = r // 2, r % 2
    xo = 1 - x
    zp, zm = (z + 1) % Z, (z + Z - 1) % Z

    def dev(ff, rr):
        return {"fsdp": ff, "rep": rr}

    up, down = dev(zp * X + x, r), dev(zm * X + x, r)
    across = dev(z * X + xo, r)
    mate = dev(f, y * 2 + 1 - c)

    twin = dev(f, (1 - y) * 2 + c)

    loads = []
    for i, (src, dst) in enumerate(
        (
            (ra, full.at[0, pl.ds(pl.multiple_of(f * rows, rows), rows), :]),
            (ea, full.at[1, pl.ds(pl.multiple_of(f * rows, rows), rows), :]),
            (rb, full.at[2, pl.ds(pl.multiple_of(f * rows, rows), rows), :]),
            (eb, full.at[3, pl.ds(pl.multiple_of(f * rows, rows), rows), :]),
            (base_in, base),
            (gout_in, gout),
            (lin_in, own.at[0, 0]),
        )
    ):
        copy = pltpu.make_async_copy(src, dst, load_sem.at[i])
        copy.start()
        loads.append(copy)

    barrier = pltpu.get_barrier_semaphore()
    friends = [up, down, across, mate, twin]
    for friend in friends:
        pl.semaphore_signal(barrier, inc=1, device_id=friend, device_id_type=MESH)
    pl.semaphore_wait(barrier, len(friends))
    for copy in loads[:4]:
        copy.wait()

    sent = []

    def guarded(cond, action):
        if cond is None:
            action()
        else:
            pl.when(cond)(action)

    def also(one, two):
        return one if two is None else two if one is None else jnp.logical_and(one, two)

    def slot(zz, xx):
        return (zz + 2 * Z) % Z * X + xx

    def piece(w, zz, xx, h):
        start = slot(zz, xx) * rows + h * half
        return full.at[w, pl.ds(pl.multiple_of(start, half), half), :]

    def relay(cond, k, zz, xx, h, ssem, rsem, target):
        ref = piece(2 * c + k, zz, xx, h)
        copy = pltpu.make_async_remote_copy(
            src_ref=ref, dst_ref=ref, send_sem=ssem, recv_sem=rsem,
            device_id=target, device_id_type=MESH,
        )
        guarded(cond, copy.start)
        sent.append((cond, copy))

    def zsend(cond, zz, h, upward):
        o = slot(zz, x)
        relay(cond, y, zz, x, h, ag_z.at[upward, o, h], ag_recv.at[y, o, h], up if upward else down)

    def xsend(cond, k, zz, h):
        o = slot(zz, x)
        relay(cond, k, zz, x, h, ag_x.at[k, o, h], ag_recv.at[k, o, h], across)

    def ysend(cond, zz, xx, h):
        o = slot(zz, xx)
        relay(cond, y, zz, xx, h, ag_y.at[y, o, h], ag_recv.at[y, o, h], twin)

    def dsend(cond, k, zz, xx, h):
        o = slot(zz, xx)
        relay(cond, k, zz, xx, h, ag_d.at[k, o, h], ag_drecv.at[k, o, h], mate)

    def arrive(cond, k, zz, xx, h):
        o = slot(zz, xx)
        ref = piece(2 * c + k, zz, xx, h)
        copy = pltpu.make_async_remote_copy(
            src_ref=ref, dst_ref=ref, send_sem=ag_d.at[k, o, h], recv_sem=ag_recv.at[k, o, h],
            device_id=mate, device_id_type=MESH,
        )
        guarded(cond, copy.wait_recv)

    def levels(d):
        if d < 0 or d >= Z:
            return []
        if d == 0:
            return [(z, None, None)]
        return [(z - d, z >= d, True), (z + d, z + d < Z, False)]

    not_top, not_bottom = z < Z - 1, z > 0
    yo = 1 - y

    def stage_line(d):
        for h in range(2):
            for zz, cond, upward in levels(d):
                if d == 0:
                    zsend(not_top, zz, h, 1)
                    zsend(not_bottom, zz, h, 0)
                else:
                    arrive(cond, y, zz, x, h)
                    if d < Z - 1:
                        zsend(also(cond, not_top if upward else not_bottom), zz, h, 1 if upward else 0)
                xsend(cond, y, zz, h)
                if d == 0:
                    if h == 1:
                        xsend(cond, yo, zz, h)
                else:
                    ysend(cond, zz, x, h)
                    dsend(cond, y, zz, x, h)

    def stage_side(d):
        for h in range(2):
            for zz, cond, _ in levels(d):
                arrive(cond, y, zz, xo, h)
                if h == 0:
                    ysend(cond, zz, xo, h)
                dsend(cond, y, zz, xo, h)
                if d > 0:
                    arrive(cond, yo, zz, x, h)
                    if h == 1:
                        xsend(cond, yo, zz, h)
                    dsend(cond, yo, zz, x, h)

    def stage_corner(d):
        for h in range(2):
            for zz, cond, _ in levels(d):
                arrive(cond, yo, zz, xo, h)
                dsend(cond, yo, zz, xo, h)

    stage_line(0)

    for copy in loads[4:]:
        copy.wait()
    tile = min(512, D)

    @pl.loop(0, D // tile)
    def _(t):
        cols = pl.ds(pl.multiple_of(t * tile, tile), tile)
        own[1, 1, :, cols] = (gout[:, cols].astype(F32) * base[:, cols].astype(F32)).astype(BF16)

    for d in range(1, Z + 2):
        if d < Z:
            stage_line(d)
        stage_side(d - 1)
        stage_corner(d - 2)
    for d in range(Z):
        for zz, cond, _ in levels(d):
            for k in range(2):
                for h in range(2):
                    for near in (True, False):
                        if near and d == 0:
                            continue
                        xx = x if near else xo
                        o = slot(zz, xx)
                        ref = piece(2 * (1 - c) + k, zz, xx, h)
                        copy = pltpu.make_async_remote_copy(
                            src_ref=ref, dst_ref=ref, send_sem=ag_d.at[k, o, h],
                            recv_sem=ag_drecv.at[k, o, h], device_id=mate, device_id_type=MESH,
                        )
                        guarded(cond, copy.wait_recv)
    for cond, copy in sent:
        guarded(cond, copy.wait_send)

    nar[0, 1] = dot_nn(own[0, 0], full[0]).astype(BF16)
    nar[1, 0] = dot_nn(own[1, 1], full[3]).astype(BF16)

    @pl.loop(0, D // tile)
    def _(t):
        cols = pl.ds(pl.multiple_of(t * tile, tile), tile)
        wide = base[:, cols].astype(F32)
        crossed = dot_nt(nar[0, 1], full[1, cols, :])
        cross_a[:, cols] = crossed
        own[1, 0, :, cols] = (own[0, 0, :, cols].astype(F32) + wide * crossed).astype(BF16)
        passed = (gout[:, cols].astype(F32) + dot_nt(nar[1, 0], full[2, cols, :])).astype(BF16)
        gmid[:, cols] = passed
        own[0, 1, :, cols] = (passed.astype(F32) * wide).astype(BF16)

    nar[1, 1] = dot_nn(own[1, 0], full[2]).astype(BF16)
    nar[0, 0] = dot_nn(own[0, 1], full[1]).astype(BF16)

    swaps = []
    for k in range(2):
        for src, dst, sem in ((own, peer_wide, pw_sem), (nar, peer_nar, pn_sem)):
            copy = pltpu.make_async_remote_copy(
                src_ref=src.at[1 - c, k], dst_ref=dst.at[k], send_sem=sem.at[0, k],
                recv_sem=sem.at[1, k], device_id=mate, device_id_type=MESH,
            )
            copy.start()
            swaps.append(copy)

    def push(src, dst, sems, target):
        copy = pltpu.make_async_remote_copy(
            src_ref=src, dst_ref=dst, send_sem=sems[0], recv_sem=sems[1],
            device_id=target, device_id_type=MESH,
        )
        copy.start()
        return copy

    for copy in swaps:
        copy.wait()
    level_rows = X * rows

    def products(o):
        cols = pl.ds(pl.multiple_of(o * level_rows, level_rows), level_rows)
        for k in range(2):
            part[k, cols, :] = dot_tn(own[c, k, :, cols], nar[c, k]) + dot_tn(
                peer_wide[k, :, cols], peer_nar[k]
            )

    def mine(k, o, xx, h):
        start = (o * X + xx) * rows + h * half
        return part[k, pl.ds(pl.multiple_of(start, half), half), :]

    flipped = z >= Z // 2
    near_end = jnp.where(flipped, Z - 1 - z, z)

    def owner(i):
        if i == Z - 1:
            return z
        j = Z - 1 - i
        o = jnp.where(j > near_end, j, j - 1)
        return jnp.where(flipped, Z - 1 - o, o)

    sums, waits = [], []

    def first(i):
        o = owner(i)
        products(o)
        for xx in range(2):
            y1_send[o, xx] = mine(yo, o, xx, 0).astype(BF16)
        one = push(y1_send.at[o], y1_recv.at[o], (y1_sem.at[0, o], y1_sem.at[1, o]), twin)
        for k in range(2):
            x1_send[o, k] = mine(k, o, xo, 1).astype(BF16)
        two = push(x1_send.at[o], x1_recv.at[o], (x1_sem.at[0, o], x1_sem.at[1, o]), across)
        waits.extend((one, two))
        sums.append([one, two])

    def second(i):
        o = owner(i)
        one, two = sums[i]
        one.wait_recv()
        x2_send[o] = (mine(y, o, xo, 0) + y1_recv[o, xo].astype(F32)).astype(BF16)
        three = push(x2_send.at[o], x2_recv.at[o], (x2_sem.at[0, o], x2_sem.at[1, o]), across)
        two.wait_recv()
        y2_send[o] = (mine(yo, o, x, 1) + x1_recv[o, yo].astype(F32)).astype(BF16)
        four = push(y2_send.at[o], y2_recv.at[o], (y2_sem.at[0, o], y2_sem.at[1, o]), twin)
        waits.extend((three, four))
        sums[i] = (three, four)

    def level_sum(o, h):
        if h == 0:
            return mine(y, o, x, 0) + y1_recv[o, x].astype(F32) + x2_recv[o].astype(F32)
        return mine(y, o, x, 1) + x1_recv[o, y].astype(F32) + y2_recv[o].astype(F32)

    def line(o, h, way, target):
        return pltpu.make_async_remote_copy(
            src_ref=z_send.at[o, h], dst_ref=z_recv.at[way, o, h], send_sem=zs_sem.at[o, h],
            recv_sem=zr_sem.at[way, o, h], device_id=target, device_id_type=MESH,
        )

    def third(i):
        o = owner(i)
        way = jnp.where(o > z, 0, 1)
        target = dev((z + 1 - 2 * way) * X + x, r)
        fed = jnp.where(o > z, z, Z - 1 - z) > 0
        for h in range(2):
            sums[i][h].wait_recv()
            value = level_sum(o, h)
            copy = line(o, h, way, target)

            @pl.when(fed)
            def _():
                copy.wait_recv()
                z_send[o, h] = (value + z_recv[way, o, h].astype(F32)).astype(BF16)

            @pl.when(jnp.logical_not(fed))
            def _():
                z_send[o, h] = value.astype(BF16)

            copy.start()
            waits.append(copy)

    def others():
        @pl.loop(0, D // tile)
        def _(t):
            cols = pl.ds(pl.multiple_of(t * tile, tile), tile)
            held = gmid[:, cols].astype(F32)
            crossed = dot_nt(nar[1, 1], full[3, cols, :])
            gbase[:, cols] = (
                gout[:, cols].astype(F32) * crossed + held * cross_a[:, cols]
            ).astype(BF16)
            gli[:, cols] = (held + dot_nt(nar[0, 0], full[0, cols, :])).astype(BF16)

    outs = []
    for i in range(Z + 1):
        if i < Z:
            first(i)
        if i == min(1, Z - 1):
            others()
            for n, (src, dst) in enumerate(((gli, gli_out), (gbase, gbase_out))):
                copy = pltpu.make_async_copy(src, dst, out_sem.at[n])
                copy.start()
                outs.append(copy)
        if 1 <= i:
            second(i - 1)
        if 2 <= i:
            third(i - 2)

    hy = []
    for h in range(2):
        sums[Z - 1][h].wait_recv()
        last_sum[h] = level_sum(z, h)
        for way, cond in ((0, not_bottom), (1, not_top)):

            @pl.when(cond)
            def _():
                line(z, h, way, across).wait_recv()
                last_sum[h] = last_sum[h] + z_recv[way, z, h].astype(F32)

        fin[y, h] = last_sum[h].astype(BF16)
        hy.append(push(fin.at[y, h], fin.at[y, h], (y_ssem.at[y, h], y_rsem.at[y, h]), twin))
    hg = []

    def hand_over(k, h):
        grads[2 * c + k, pl.ds(h * half, half), :] = fin[k, h].astype(F32) * factor
        ref = grads.at[2 * c + k, pl.ds(h * half, half), :]
        hg.append(push(ref, ref, (g_sem.at[0, k, h], g_sem.at[1, k, h]), mate))

    for h in range(2):
        hand_over(y, h)
    for h in range(2):
        pltpu.make_async_remote_copy(
            src_ref=fin.at[yo, h], dst_ref=fin.at[yo, h], send_sem=y_ssem.at[yo, h],
            recv_sem=y_rsem.at[yo, h], device_id=twin, device_id_type=MESH,
        ).wait_recv()
        hand_over(yo, h)
    for k in range(2):
        for h in range(2):
            ref = grads.at[2 * (1 - c) + k, pl.ds(h * half, half), :]
            pltpu.make_async_remote_copy(
                src_ref=ref, dst_ref=ref, send_sem=g_sem.at[0, k, h],
                recv_sem=g_sem.at[1, k, h], device_id=mate, device_id_type=MESH,
            ).wait_recv()
    last = pltpu.make_async_copy(grads, grads_out, out_sem.at[2])
    last.start()
    for copy in waits + hy + hg:
        copy.wait_send()
    for copy in outs + [last]:
        copy.wait()


def solution(mesh):
    F, R = mesh.shape["fsdp"], mesh.shape["rep"]
    X = 2
    Z = F // X
    assert R == 4 and F % X == 0

    def on_device(base, lin, gout, ra, ea, rb, eb):
        T, D = base.shape
        rows, K = ra.shape
        half = rows // 2
        factor = 1.0 / math.sqrt(T * F * R)
        dma = pltpu.SemaphoreType.DMA
        vm = pltpu.VMEM
        any_spec = pl.BlockSpec(memory_space=pl.ANY)
        gli, gbase, grads = pl.pallas_call(
            functools.partial(kernel, F, R, factor),
            out_shape=(
                jax.ShapeDtypeStruct((T, D), BF16),
                jax.ShapeDtypeStruct((T, D), BF16),
                jax.ShapeDtypeStruct((4, rows, K), F32),
            ),
            in_specs=[any_spec] * 7,
            out_specs=[any_spec] * 3,
            scratch_shapes=[
                vm((T, D), BF16),
                vm((T, D), BF16),
                vm((2, 2, T, D), BF16),
                vm((2, 2, T, K), BF16),
                vm((2, T, D), BF16),
                vm((2, T, K), BF16),
                vm((4, D, K), BF16),
                vm((T, D), F32),
                vm((T, D), BF16),
                vm((T, D), BF16),
                vm((T, D), BF16),
                vm((2, D, K), F32),
                vm((4, rows, K), F32),
                vm((Z, 2, half, K), BF16),
                vm((Z, 2, half, K), BF16),
                vm((Z, 2, half, K), BF16),
                vm((Z, 2, half, K), BF16),
                vm((Z, half, K), BF16),
                vm((Z, half, K), BF16),
                vm((Z, half, K), BF16),
                vm((Z, half, K), BF16),
                vm((Z, 2, half, K), BF16),
                vm((2, Z, 2, half, K), BF16),
                vm((2, half, K), F32),
                vm((2, 2, half, K), BF16),
                dma((7,)),
                dma((3,)),
                dma((2, F, 2)),
                dma((2, F, 2)),
                dma((2, F, 2)),
                dma((2, F, 2)),
                dma((2, F, 2)),
                dma((2, F, 2)),
                dma((2, 2)),
                dma((2, 2)),
                dma((2, Z)),
                dma((2, Z)),
                dma((2, Z)),
                dma((2, Z)),
                dma((Z, 2)),
                dma((2, Z, 2)),
                dma((2, 2)),
                dma((2, 2)),
                dma((2, 2, 2)),
            ],
            compiler_params=pltpu.CompilerParams(
                collective_id=1, has_side_effects=True, vmem_limit_bytes=60 * 1024 * 1024
            ),
        )(base, lin, gout, ra, ea, rb, eb)
        return gli, gbase, grads[0], grads[1], grads[2], grads[3]

    both = P(("fsdp", "rep"), None)
    one = P("fsdp", None)
    return jax.shard_map(
        on_device,
        mesh=mesh,
        in_specs=(both, both, both, one, one, one, one),
        out_specs=(both, both, one, one, one, one),
        check_vma=False,
    )
```

```python
import functools
import math

import jax
import jax.numpy as jnp
from jax import lax
from jax.experimental import pallas as pl
from jax.experimental.pallas import tpu as pltpu
from jax.sharding import PartitionSpec as P

MESH = pl.DeviceIdType.MESH
F32 = jnp.float32
BF16 = jnp.bfloat16


def dot_nn(left, right):
    return lax.dot_general(left, right, (((1,), (0,)), ((), ())), preferred_element_type=F32)


def dot_nt(left, right):
    return lax.dot_general(left, right, (((1,), (1,)), ((), ())), preferred_element_type=F32)


def dot_tn(left, right):
    return lax.dot_general(left, right, (((0,), (0,)), ((), ())), preferred_element_type=F32)


def kernel(
    F,
    R,
    base_in,
    lin_in,
    gout_in,
    ra,
    ea,
    rb,
    eb,
    gli_out,
    gbase_out,
    grads_out,
    base,
    gout,
    own,
    nar,
    peer_wide,
    peer_nar,
    full,
    cross_a,
    gmid,
    gli,
    gbase,
    part,
    grads,
    y1_send,
    y1_recv,
    x1_send,
    x1_recv,
    x2_send,
    x2_recv,
    z_send,
    z_recv,
    last_sum,
    fin,
    load_sem,
    out_sem,
    ag_recv,
    ag_z,
    ag_x,
    ag_y,
    ag_d,
    ag_drecv,
    pw_sem,
    pn_sem,
    y1_sem,
    x1_sem,
    x2_sem,
    zs_sem,
    zr_sem,
    y_ssem,
    y_rsem,
    g_sem,
):
    X = 2
    Z = F // X
    rows = ra.shape[0]
    half = rows // 2
    D = base.shape[1]
    f = lax.axis_index("fsdp")
    r = lax.axis_index("rep")
    z, x = f // X, f % X
    y, c = r // 2, r % 2
    xo = 1 - x
    zp, zm = (z + 1) % Z, (z + Z - 1) % Z

    def dev(ff, rr):
        return {"fsdp": ff, "rep": rr}

    up, down = dev(zp * X + x, r), dev(zm * X + x, r)
    across = dev(z * X + xo, r)
    mate = dev(f, y * 2 + 1 - c)

    twin = dev(f, (1 - y) * 2 + c)

    loads = []
    for i, (src, dst) in enumerate(
        (
            (ra, full.at[0, pl.ds(pl.multiple_of(f * rows, rows), rows), :]),
            (ea, full.at[1, pl.ds(pl.multiple_of(f * rows, rows), rows), :]),
            (rb, full.at[2, pl.ds(pl.multiple_of(f * rows, rows), rows), :]),
            (eb, full.at[3, pl.ds(pl.multiple_of(f * rows, rows), rows), :]),
            (base_in, base),
            (gout_in, gout),
            (lin_in, own.at[0, 0]),
        )
    ):
        copy = pltpu.make_async_copy(src, dst, load_sem.at[i])
        copy.start()
        loads.append(copy)

    barrier = pltpu.get_barrier_semaphore()
    friends = [up, down, across, mate, twin]
    for friend in friends:
        pl.semaphore_signal(barrier, inc=1, device_id=friend, device_id_type=MESH)
    pl.semaphore_wait(barrier, len(friends))
    for copy in loads[:4]:
        copy.wait()

    def push(src, dst, sems, target):
        copy = pltpu.make_async_remote_copy(
            src_ref=src, dst_ref=dst, send_sem=sems[0], recv_sem=sems[1],
            device_id=target, device_id_type=MESH,
        )
        copy.start()
        return copy

    swaps = []

    def swap(src, dst, sem, k):
        swaps.append(push(src.at[1 - c, k], dst.at[k], (sem.at[0, k], sem.at[1, k]), mate))

    sent = []

    def guarded(cond, action):
        if cond is None:
            action()
        else:
            pl.when(cond)(action)

    def also(one, two):
        return one if two is None else two if one is None else jnp.logical_and(one, two)

    def slot(zz, xx):
        return (zz + 2 * Z) % Z * X + xx

    def piece(w, zz, xx, h):
        start = slot(zz, xx) * rows + h * half
        return full.at[w, pl.ds(pl.multiple_of(start, half), half), :]

    def relay(cond, k, zz, xx, h, ssem, rsem, target):
        ref = piece(2 * c + k, zz, xx, h)
        copy = pltpu.make_async_remote_copy(
            src_ref=ref, dst_ref=ref, send_sem=ssem, recv_sem=rsem,
            device_id=target, device_id_type=MESH,
        )
        guarded(cond, copy.start)
        sent.append((cond, copy))

    def zsend(cond, zz, h, upward):
        o = slot(zz, x)
        relay(cond, y, zz, x, h, ag_z.at[upward, o, h], ag_recv.at[y, o, h], up if upward else down)

    def xsend(cond, k, zz, h):
        o = slot(zz, x)
        relay(cond, k, zz, x, h, ag_x.at[k, o, h], ag_recv.at[k, o, h], across)

    def ysend(cond, zz, xx, h):
        o = slot(zz, xx)
        relay(cond, y, zz, xx, h, ag_y.at[y, o, h], ag_recv.at[y, o, h], twin)

    def dsend(cond, k, zz, xx, h):
        o = slot(zz, xx)
        relay(cond, k, zz, xx, h, ag_d.at[k, o, h], ag_drecv.at[k, o, h], mate)

    def arrive(cond, k, zz, xx, h):
        o = slot(zz, xx)
        ref = piece(2 * c + k, zz, xx, h)
        copy = pltpu.make_async_remote_copy(
            src_ref=ref, dst_ref=ref, send_sem=ag_d.at[k, o, h], recv_sem=ag_recv.at[k, o, h],
            device_id=mate, device_id_type=MESH,
        )
        guarded(cond, copy.wait_recv)

    def levels(d):
        if d < 0 or d >= Z:
            return []
        if d == 0:
            return [(z, None, None)]
        return [(z - d, z >= d, True), (z + d, z + d < Z, False)]

    not_top, not_bottom = z < Z - 1, z > 0
    yo = 1 - y

    def stage_line(d):
        for h in range(2):
            for zz, cond, upward in levels(d):
                if d == 0:
                    zsend(not_top, zz, h, 1)
                    zsend(not_bottom, zz, h, 0)
                else:
                    arrive(cond, y, zz, x, h)
                    if d < Z - 1:
                        zsend(also(cond, not_top if upward else not_bottom), zz, h, 1 if upward else 0)
                xsend(cond, y, zz, h)
                if d == 0:
                    if h == 1:
                        xsend(cond, yo, zz, h)
                else:
                    ysend(cond, zz, x, h)
                    dsend(cond, y, zz, x, h)

    def stage_side(d):
        for h in range(2):
            for zz, cond, _ in levels(d):
                arrive(cond, y, zz, xo, h)
                if h == 0:
                    ysend(cond, zz, xo, h)
                dsend(cond, y, zz, xo, h)
                if d > 0:
                    arrive(cond, yo, zz, x, h)
                    if h == 1:
                        xsend(cond, yo, zz, h)
                    dsend(cond, yo, zz, x, h)

    def stage_corner(d):
        for h in range(2):
            for zz, cond, _ in levels(d):
                arrive(cond, yo, zz, xo, h)
                dsend(cond, yo, zz, xo, h)

    stage_line(0)

    for copy in loads[4:]:
        copy.wait()
    tile = min(512, D)

    @pl.loop(0, D // tile)
    def _(t):
        cols = pl.ds(pl.multiple_of(t * tile, tile), tile)
        own[1, 1, :, cols] = (gout[:, cols].astype(F32) * base[:, cols].astype(F32)).astype(BF16)

    swap(own, peer_wide, pw_sem, 1 - c)
    for d in range(1, Z + 2):
        if d < Z:
            stage_line(d)
        stage_side(d - 1)
        stage_corner(d - 2)
    for d in range(Z):
        for zz, cond, _ in levels(d):
            for k in range(2):
                for h in range(2):
                    for near in (True, False):
                        if near and d == 0:
                            continue
                        xx = x if near else xo
                        o = slot(zz, xx)
                        ref = piece(2 * (1 - c) + k, zz, xx, h)
                        copy = pltpu.make_async_remote_copy(
                            src_ref=ref, dst_ref=ref, send_sem=ag_d.at[k, o, h],
                            recv_sem=ag_drecv.at[k, o, h], device_id=mate, device_id_type=MESH,
                        )
                        guarded(cond, copy.wait_recv)
    for cond, copy in sent:
        guarded(cond, copy.wait_send)

    nar[0, 1] = dot_nn(own[0, 0], full[0]).astype(BF16)
    nar[1, 0] = dot_nn(own[1, 1], full[3]).astype(BF16)

    @pl.loop(0, D // tile)
    def _(t):
        cols = pl.ds(pl.multiple_of(t * tile, tile), tile)
        wide = base[:, cols].astype(F32)
        crossed = dot_nt(nar[0, 1], full[1, cols, :])
        cross_a[:, cols] = crossed
        own[1, 0, :, cols] = (own[0, 0, :, cols].astype(F32) + wide * crossed).astype(BF16)
        passed = (gout[:, cols].astype(F32) + dot_nt(nar[1, 0], full[2, cols, :])).astype(BF16)
        gmid[:, cols] = passed
        own[0, 1, :, cols] = (passed.astype(F32) * wide).astype(BF16)

    swap(own, peer_wide, pw_sem, c)
    nar[1, 1] = dot_nn(own[1, 0], full[2]).astype(BF16)
    nar[0, 0] = dot_nn(own[0, 1], full[1]).astype(BF16)

    for k in range(2):
        swap(nar, peer_nar, pn_sem, k)
    for copy in swaps:
        copy.wait()
    level_rows = X * rows

    def products(o):
        cols = pl.ds(pl.multiple_of(o * level_rows, level_rows), level_rows)
        for k in range(2):
            part[k, cols, :] = dot_tn(own[c, k, :, cols], nar[c, k]) + dot_tn(
                peer_wide[k, :, cols], peer_nar[k]
            )

    def mine(k, o, xx, h):
        start = (o * X + xx) * rows + h * half
        return part[k, pl.ds(pl.multiple_of(start, half), half), :]

    flipped = z >= Z // 2
    near_end = jnp.where(flipped, Z - 1 - z, z)

    def owner(i):
        if i == Z - 1:
            return z
        j = Z - 1 - i
        o = jnp.where(j > near_end, j, j - 1)
        return jnp.where(flipped, Z - 1 - o, o)

    sums, waits = [], []

    def first(i):
        o = owner(i)
        products(o)
        for xx in range(2):
            y1_send[o, xx] = mine(yo, o, xx, 0).astype(BF16)
        one = push(y1_send.at[o], y1_recv.at[o], (y1_sem.at[0, o], y1_sem.at[1, o]), twin)
        for k in range(2):
            x1_send[o, k] = mine(k, o, xo, 1).astype(BF16)
        two = push(x1_send.at[o], x1_recv.at[o], (x1_sem.at[0, o], x1_sem.at[1, o]), across)
        waits.extend((one, two))
        sums.append([one, two])

    def second(i):
        o = owner(i)
        one, two = sums[i]
        one.wait_recv()
        x2_send[o] = (mine(y, o, xo, 0) + y1_recv[o, xo].astype(F32)).astype(BF16)
        three = push(x2_send.at[o], x2_recv.at[o], (x2_sem.at[0, o], x2_sem.at[1, o]), across)
        waits.append(three)
        sums[i] = (two, None, three)

    def level_sum(o, n):
        if n == 2:
            return mine(y, o, x, 0) + y1_recv[o, x].astype(F32) + x2_recv[o].astype(F32)
        return mine(n, o, x, 1) + x1_recv[o, n].astype(F32)

    def line(o, n, way, target):
        return pltpu.make_async_remote_copy(
            src_ref=z_send.at[o, n], dst_ref=z_recv.at[way, o, n], send_sem=zs_sem.at[o, n],
            recv_sem=zr_sem.at[way, o, n], device_id=target, device_id_type=MESH,
        )

    def third(i):
        o = owner(i)
        way = jnp.where(o > z, 0, 1)
        target = dev((z + 1 - 2 * way) * X + x, r)
        fed = jnp.where(o > z, z, Z - 1 - z) > 0
        for n in range(3):
            if sums[i][n] is not None:
                sums[i][n].wait_recv()
            value = level_sum(o, n)
            copy = line(o, n, way, target)

            @pl.when(fed)
            def _():
                copy.wait_recv()
                z_send[o, n] = (value + z_recv[way, o, n].astype(F32)).astype(BF16)

            @pl.when(jnp.logical_not(fed))
            def _():
                z_send[o, n] = value.astype(BF16)

            copy.start()
            waits.append(copy)

    def others():
        @pl.loop(0, D // tile)
        def _(t):
            cols = pl.ds(pl.multiple_of(t * tile, tile), tile)
            held = gmid[:, cols].astype(F32)
            crossed = dot_nt(nar[1, 1], full[3, cols, :])
            gbase[:, cols] = (
                gout[:, cols].astype(F32) * crossed + held * cross_a[:, cols]
            ).astype(BF16)
            gli[:, cols] = (held + dot_nt(nar[0, 0], full[0, cols, :])).astype(BF16)

    outs = []
    for i in range(Z + 1):
        if i < Z:
            first(i)
        if i == min(1, Z - 1):
            others()
            for n, (src, dst) in enumerate(((gli, gli_out), (gbase, gbase_out))):
                copy = pltpu.make_async_copy(src, dst, out_sem.at[n])
                copy.start()
                outs.append(copy)
        if 1 <= i:
            second(i - 1)
        if 2 <= i:
            third(i - 2)

    hy = []
    for n in range(3):
        if sums[Z - 1][n] is not None:
            sums[Z - 1][n].wait_recv()
        last_sum[n] = level_sum(z, n)
        for way, cond in ((0, not_bottom), (1, not_top)):

            @pl.when(cond)
            def _():
                line(z, n, way, across).wait_recv()
                last_sum[n] = last_sum[n] + z_recv[way, z, n].astype(F32)

        fin[y, n] = last_sum[n].astype(BF16)
        hy.append(push(fin.at[y, n], fin.at[y, n], (y_ssem.at[y, n], y_rsem.at[y, n]), twin))
    hg = []

    def hand_over(k, h, value):
        grads[2 * c + k, pl.ds(h * half, half), :] = value
        ref = grads.at[2 * c + k, pl.ds(h * half, half), :]
        hg.append(push(ref, ref, (g_sem.at[0, k, h], g_sem.at[1, k, h]), mate))

    hand_over(y, 0, fin[y, 2])
    for n in range(3):
        pltpu.make_async_remote_copy(
            src_ref=fin.at[yo, n], dst_ref=fin.at[yo, n], send_sem=y_ssem.at[yo, n],
            recv_sem=y_rsem.at[yo, n], device_id=twin, device_id_type=MESH,
        ).wait_recv()
        if n < 2:
            hand_over(n, 1, (fin[0, n].astype(F32) + fin[1, n].astype(F32)).astype(BF16))
        else:
            hand_over(yo, 0, fin[yo, 2])
    for k in range(2):
        for h in range(2):
            ref = grads.at[2 * (1 - c) + k, pl.ds(h * half, half), :]
            pltpu.make_async_remote_copy(
                src_ref=ref, dst_ref=ref, send_sem=g_sem.at[0, k, h],
                recv_sem=g_sem.at[1, k, h], device_id=mate, device_id_type=MESH,
            ).wait_recv()
    last = pltpu.make_async_copy(grads, grads_out, out_sem.at[2])
    last.start()
    for copy in waits + hy + hg:
        copy.wait_send()
    for copy in outs + [last]:
        copy.wait()


def solution(mesh):
    F, R = mesh.shape["fsdp"], mesh.shape["rep"]
    X = 2
    Z = F // X
    assert R == 4 and F % X == 0

    def on_device(base, lin, gout, ra, ea, rb, eb):
        T, D = base.shape
        rows, K = ra.shape
        half = rows // 2
        factor = 1.0 / math.sqrt(T * F * R)
        dma = pltpu.SemaphoreType.DMA
        vm = pltpu.VMEM
        any_spec = pl.BlockSpec(memory_space=pl.ANY)
        gli, gbase, grads = pl.pallas_call(
            functools.partial(kernel, F, R),
            out_shape=(
                jax.ShapeDtypeStruct((T, D), BF16),
                jax.ShapeDtypeStruct((T, D), BF16),
                jax.ShapeDtypeStruct((4, rows, K), BF16),
            ),
            in_specs=[any_spec] * 7,
            out_specs=[any_spec] * 3,
            scratch_shapes=[
                vm((T, D), BF16),
                vm((T, D), BF16),
                vm((2, 2, T, D), BF16),
                vm((2, 2, T, K), BF16),
                vm((2, T, D), BF16),
                vm((2, T, K), BF16),
                vm((4, D, K), BF16),
                vm((T, D), F32),
                vm((T, D), BF16),
                vm((T, D), BF16),
                vm((T, D), BF16),
                vm((2, D, K), F32),
                vm((4, rows, K), BF16),
                vm((Z, 2, half, K), BF16),
                vm((Z, 2, half, K), BF16),
                vm((Z, 2, half, K), BF16),
                vm((Z, 2, half, K), BF16),
                vm((Z, half, K), BF16),
                vm((Z, half, K), BF16),
                vm((Z, 3, half, K), BF16),
                vm((2, Z, 3, half, K), BF16),
                vm((3, half, K), F32),
                vm((2, 3, half, K), BF16),
                dma((7,)),
                dma((3,)),
                dma((2, F, 2)),
                dma((2, F, 2)),
                dma((2, F, 2)),
                dma((2, F, 2)),
                dma((2, F, 2)),
                dma((2, F, 2)),
                dma((2, 2)),
                dma((2, 2)),
                dma((2, Z)),
                dma((2, Z)),
                dma((2, Z)),
                dma((Z, 3)),
                dma((2, Z, 3)),
                dma((2, 3)),
                dma((2, 3)),
                dma((2, 2, 2)),
            ],
            compiler_params=pltpu.CompilerParams(
                collective_id=1, has_side_effects=True, vmem_limit_bytes=60 * 1024 * 1024
            ),
        )(base, lin, gout, ra, ea, rb, eb)
        scaled = [grads[w].astype(F32) * factor for w in range(4)]
        return (gli, gbase, *scaled)

    both = P(("fsdp", "rep"), None)
    one = P("fsdp", None)
    return jax.shard_map(
        on_device,
        mesh=mesh,
        in_specs=(both, both, both, one, one, one, one),
        out_specs=(both, both, one, one, one, one),
        check_vma=False,
    )
```

```python
import functools
import math

import jax
import jax.numpy as jnp
from jax import lax
from jax.experimental import pallas as pl
from jax.experimental.pallas import tpu as pltpu
from jax.sharding import PartitionSpec as P

MESH = pl.DeviceIdType.MESH
F32 = jnp.float32
BF16 = jnp.bfloat16


def dot_nn(left, right):
    return lax.dot_general(left, right, (((1,), (0,)), ((), ())), preferred_element_type=F32)


def dot_nt(left, right):
    return lax.dot_general(left, right, (((1,), (1,)), ((), ())), preferred_element_type=F32)


def dot_tn(left, right):
    return lax.dot_general(left, right, (((0,), (0,)), ((), ())), preferred_element_type=F32)


def kernel(
    F,
    R,
    base_in,
    lin_in,
    gout_in,
    ra,
    ea,
    rb,
    eb,
    gli_out,
    gbase_out,
    grads_out,
    base,
    gout,
    own,
    nar,
    peer_wide,
    peer_nar,
    full,
    cross_a,
    gmid,
    gli,
    gbase,
    part,
    grads,
    y1_send,
    y1_recv,
    x1_send,
    x1_recv,
    x2_send,
    x2_recv,
    z_send,
    z_recv,
    last_sum,
    fin,
    load_sem,
    out_sem,
    ag_recv,
    ag_z,
    ag_x,
    ag_y,
    ag_d,
    ag_drecv,
    pw_sem,
    pn_sem,
    y1_sem,
    x1_sem,
    x2_sem,
    zs_sem,
    zr_sem,
    y_ssem,
    y_rsem,
    g_sem,
):
    X = 2
    Z = F // X
    rows = ra.shape[0]
    half = rows // 2
    D = base.shape[1]
    f = lax.axis_index("fsdp")
    r = lax.axis_index("rep")
    z, x = f // X, f % X
    y, c = r // 2, r % 2
    xo = 1 - x
    zp, zm = (z + 1) % Z, (z + Z - 1) % Z

    def dev(ff, rr):
        return {"fsdp": ff, "rep": rr}

    up, down = dev(zp * X + x, r), dev(zm * X + x, r)
    across = dev(z * X + xo, r)
    mate = dev(f, y * 2 + 1 - c)

    twin = dev(f, (1 - y) * 2 + c)

    loads = []
    for i, (src, dst) in enumerate(
        (
            (ra, full.at[0, pl.ds(pl.multiple_of(f * rows, rows), rows), :]),
            (ea, full.at[1, pl.ds(pl.multiple_of(f * rows, rows), rows), :]),
            (rb, full.at[2, pl.ds(pl.multiple_of(f * rows, rows), rows), :]),
            (eb, full.at[3, pl.ds(pl.multiple_of(f * rows, rows), rows), :]),
            (base_in, base),
            (gout_in, gout),
            (lin_in, own.at[0, 0]),
        )
    ):
        copy = pltpu.make_async_copy(src, dst, load_sem.at[i])
        copy.start()
        loads.append(copy)

    barrier = pltpu.get_barrier_semaphore()
    friends = [up, down, across, mate, twin]
    for friend in friends:
        pl.semaphore_signal(barrier, inc=1, device_id=friend, device_id_type=MESH)
    pl.semaphore_wait(barrier, len(friends))
    for copy in loads[:4]:
        copy.wait()

    def push(src, dst, sems, target):
        copy = pltpu.make_async_remote_copy(
            src_ref=src, dst_ref=dst, send_sem=sems[0], recv_sem=sems[1],
            device_id=target, device_id_type=MESH,
        )
        copy.start()
        return copy

    swaps = []

    def swap(src, dst, sem, k):
        swaps.append(push(src.at[1 - c, k], dst.at[k], (sem.at[0, k], sem.at[1, k]), mate))

    sent = []

    def guarded(cond, action):
        if cond is None:
            action()
        else:
            pl.when(cond)(action)

    def also(one, two):
        return one if two is None else two if one is None else jnp.logical_and(one, two)

    def slot(zz, xx):
        return (zz + 2 * Z) % Z * X + xx

    def piece(w, zz, xx, h):
        start = slot(zz, xx) * rows + h * half
        return full.at[w, pl.ds(pl.multiple_of(start, half), half), :]

    def relay(cond, k, zz, xx, h, ssem, rsem, target):
        ref = piece(2 * c + k, zz, xx, h)
        copy = pltpu.make_async_remote_copy(
            src_ref=ref, dst_ref=ref, send_sem=ssem, recv_sem=rsem,
            device_id=target, device_id_type=MESH,
        )
        guarded(cond, copy.start)
        sent.append((cond, copy))

    def zsend(cond, zz, xx, h, upward):
        o = slot(zz, xx)
        relay(cond, y, zz, xx, h, ag_z.at[upward, o, h], ag_recv.at[y, o, h], up if upward else down)

    def xsend(cond, k, zz, h):
        o = slot(zz, x)
        relay(cond, k, zz, x, h, ag_x.at[k, o, h], ag_recv.at[k, o, h], across)

    def ysend(cond, zz, xx, h):
        o = slot(zz, xx)
        relay(cond, y, zz, xx, h, ag_y.at[y, o, h], ag_recv.at[y, o, h], twin)

    def dsend(cond, k, zz, xx, h):
        o = slot(zz, xx)
        relay(cond, k, zz, xx, h, ag_d.at[k, o, h], ag_drecv.at[k, o, h], mate)

    def arrive(cond, k, zz, xx, h):
        o = slot(zz, xx)
        ref = piece(2 * c + k, zz, xx, h)
        copy = pltpu.make_async_remote_copy(
            src_ref=ref, dst_ref=ref, send_sem=ag_d.at[k, o, h], recv_sem=ag_recv.at[k, o, h],
            device_id=mate, device_id_type=MESH,
        )
        guarded(cond, copy.wait_recv)

    def levels(d):
        if d < 0 or d >= Z:
            return []
        if d == 0:
            return [(z, None, None)]
        return [(z - d, z >= d, True), (z + d, z + d < Z, False)]

    not_top, not_bottom = z < Z - 1, z > 0
    yo = 1 - y

    def along(d, cond, zz, xx, h, upward):
        if d == 0:
            zsend(not_top, zz, xx, h, 1)
            zsend(not_bottom, zz, xx, h, 0)
        elif d < Z - 1:
            zsend(also(cond, not_top if upward else not_bottom), zz, xx, h, 1 if upward else 0)

    def stage_line(d):
        for h in (1, 0):
            for zz, cond, upward in levels(d):
                if d > 0:
                    arrive(cond, y, zz, x, h)
                along(d, cond, zz, x, h, upward)
                if d == 0 or h == 0:
                    xsend(cond, y, zz, h)
                if d > 0:
                    ysend(cond, zz, x, h)
                    dsend(cond, y, zz, x, h)
        if d == 0:
            xsend(None, yo, z, 1)

    def stage_other(d):
        for zz, cond, upward in levels(d):
            arrive(cond, y, zz, xo, 1)
            along(d, cond, zz, xo, 1, upward)
            if d > 1:
                ysend(cond, zz, xo, 1)
            dsend(cond, y, zz, xo, 1)

    def stage_side(d):
        for zz, cond, _ in levels(d):
            arrive(cond, y, zz, xo, 0)
            if d == 0:
                ysend(cond, zz, xo, 0)
            dsend(cond, y, zz, xo, 0)
        if d > 0:
            for h in (1, 0):
                for zz, cond, _ in levels(d):
                    arrive(cond, yo, zz, x, h)
                    if h == 0 or d == 1:
                        xsend(cond, yo, zz, h)
                    dsend(cond, yo, zz, x, h)

    def stage_corner(d):
        for h in range(2):
            for zz, cond, _ in levels(d):
                arrive(cond, yo, zz, xo, h)
                dsend(cond, yo, zz, xo, h)

    stage_line(0)

    for copy in loads[4:]:
        copy.wait()
    tile = min(512, D)

    @pl.loop(0, D // tile)
    def _(t):
        cols = pl.ds(pl.multiple_of(t * tile, tile), tile)
        own[1, 1, :, cols] = (gout[:, cols].astype(F32) * base[:, cols].astype(F32)).astype(BF16)

    swap(own, peer_wide, pw_sem, 1 - c)
    for d in range(1, Z + 2):
        if d == 1:
            stage_other(0)
        if d < Z:
            stage_line(d)
        if d > 1 and d - 1 < Z:
            stage_other(d - 1)
        stage_side(d - 1)
        stage_corner(d - 2)
    for d in range(Z):
        for zz, cond, _ in levels(d):
            for k in range(2):
                for h in range(2):
                    for near in (True, False):
                        if near and d == 0:
                            continue
                        xx = x if near else xo
                        o = slot(zz, xx)
                        ref = piece(2 * (1 - c) + k, zz, xx, h)
                        copy = pltpu.make_async_remote_copy(
                            src_ref=ref, dst_ref=ref, send_sem=ag_d.at[k, o, h],
                            recv_sem=ag_drecv.at[k, o, h], device_id=mate, device_id_type=MESH,
                        )
                        guarded(cond, copy.wait_recv)
    for cond, copy in sent:
        guarded(cond, copy.wait_send)

    nar[0, 1] = dot_nn(own[0, 0], full[0]).astype(BF16)
    nar[1, 0] = dot_nn(own[1, 1], full[3]).astype(BF16)

    @pl.loop(0, D // tile)
    def _(t):
        cols = pl.ds(pl.multiple_of(t * tile, tile), tile)
        wide = base[:, cols].astype(F32)
        crossed = dot_nt(nar[0, 1], full[1, cols, :])
        cross_a[:, cols] = crossed
        own[1, 0, :, cols] = (own[0, 0, :, cols].astype(F32) + wide * crossed).astype(BF16)
        passed = (gout[:, cols].astype(F32) + dot_nt(nar[1, 0], full[2, cols, :])).astype(BF16)
        gmid[:, cols] = passed
        own[0, 1, :, cols] = (passed.astype(F32) * wide).astype(BF16)

    swap(own, peer_wide, pw_sem, c)
    nar[1, 1] = dot_nn(own[1, 0], full[2]).astype(BF16)
    nar[0, 0] = dot_nn(own[0, 1], full[1]).astype(BF16)

    for k in range(2):
        swap(nar, peer_nar, pn_sem, k)
    for copy in swaps:
        copy.wait()
    level_rows = X * rows

    def products(o):
        cols = pl.ds(pl.multiple_of(o * level_rows, level_rows), level_rows)
        for k in range(2):
            part[k, cols, :] = dot_tn(own[c, k, :, cols], nar[c, k]) + dot_tn(
                peer_wide[k, :, cols], peer_nar[k]
            )

    def mine(k, o, xx, h):
        start = (o * X + xx) * rows + h * half
        return part[k, pl.ds(pl.multiple_of(start, half), half), :]

    flipped = z >= Z // 2
    near_end = jnp.where(flipped, Z - 1 - z, z)

    def owner(i):
        if i == Z - 1:
            return z
        j = Z - 1 - i
        o = jnp.where(j > near_end, j, j - 1)
        return jnp.where(flipped, Z - 1 - o, o)

    sums, waits = [], []

    def first(i):
        o = owner(i)
        products(o)
        for xx in range(2):
            y1_send[o, xx] = mine(yo, o, xx, 0).astype(BF16)
        one = push(y1_send.at[o], y1_recv.at[o], (y1_sem.at[0, o], y1_sem.at[1, o]), twin)
        for k in range(2):
            x1_send[o, k] = mine(k, o, xo, 1).astype(BF16)
        two = push(x1_send.at[o], x1_recv.at[o], (x1_sem.at[0, o], x1_sem.at[1, o]), across)
        waits.extend((one, two))
        sums.append([one, two])

    def second(i):
        o = owner(i)
        one, two = sums[i]
        one.wait_recv()
        x2_send[o] = (mine(y, o, xo, 0) + y1_recv[o, xo].astype(F32)).astype(BF16)
        three = push(x2_send.at[o], x2_recv.at[o], (x2_sem.at[0, o], x2_sem.at[1, o]), across)
        waits.append(three)
        sums[i] = (two, None, three)

    def level_sum(o, n):
        if n == 2:
            return mine(y, o, x, 0) + y1_recv[o, x].astype(F32) + x2_recv[o].astype(F32)
        return mine(n, o, x, 1) + x1_recv[o, n].astype(F32)

    def line(o, n, way, target):
        return pltpu.make_async_remote_copy(
            src_ref=z_send.at[o, n], dst_ref=z_recv.at[way, o, n], send_sem=zs_sem.at[o, n],
            recv_sem=zr_sem.at[way, o, n], device_id=target, device_id_type=MESH,
        )

    def third(i):
        o = owner(i)
        way = jnp.where(o > z, 0, 1)
        target = dev((z + 1 - 2 * way) * X + x, r)
        fed = jnp.where(o > z, z, Z - 1 - z) > 0
        for n in range(3):
            if sums[i][n] is not None:
                sums[i][n].wait_recv()
            value = level_sum(o, n)
            copy = line(o, n, way, target)

            @pl.when(fed)
            def _():
                copy.wait_recv()
                z_send[o, n] = (value + z_recv[way, o, n].astype(F32)).astype(BF16)

            @pl.when(jnp.logical_not(fed))
            def _():
                z_send[o, n] = value.astype(BF16)

            copy.start()
            waits.append(copy)

    def others():
        @pl.loop(0, D // tile)
        def _(t):
            cols = pl.ds(pl.multiple_of(t * tile, tile), tile)
            held = gmid[:, cols].astype(F32)
            crossed = dot_nt(nar[1, 1], full[3, cols, :])
            gbase[:, cols] = (
                gout[:, cols].astype(F32) * crossed + held * cross_a[:, cols]
            ).astype(BF16)
            gli[:, cols] = (held + dot_nt(nar[0, 0], full[0, cols, :])).astype(BF16)

    outs = []
    for i in range(Z - 1):
        first(i)
        if i > 0:
            second(i - 1)
            if i > 1:
                third(i - 2)
    second(Z - 2)
    first(Z - 1)
    others()
    for n, (src, dst) in enumerate(((gli, gli_out), (gbase, gbase_out))):
        copy = pltpu.make_async_copy(src, dst, out_sem.at[n])
        copy.start()
        outs.append(copy)
    second(Z - 1)
    for i in range(max(Z - 3, 0), Z - 1):
        third(i)

    hy = []
    for n in range(3):
        if sums[Z - 1][n] is not None:
            sums[Z - 1][n].wait_recv()
        last_sum[n] = level_sum(z, n)
        for way, cond in ((0, not_bottom), (1, not_top)):

            @pl.when(cond)
            def _():
                line(z, n, way, across).wait_recv()
                last_sum[n] = last_sum[n] + z_recv[way, z, n].astype(F32)

        fin[y, n] = last_sum[n].astype(BF16)
        hy.append(push(fin.at[y, n], fin.at[y, n], (y_ssem.at[y, n], y_rsem.at[y, n]), twin))
    hg = []

    def hand_over(k, h, value):
        grads[2 * c + k, pl.ds(h * half, half), :] = value
        ref = grads.at[2 * c + k, pl.ds(h * half, half), :]
        hg.append(push(ref, ref, (g_sem.at[0, k, h], g_sem.at[1, k, h]), mate))

    hand_over(y, 0, fin[y, 2])
    for n in range(3):
        pltpu.make_async_remote_copy(
            src_ref=fin.at[yo, n], dst_ref=fin.at[yo, n], send_sem=y_ssem.at[yo, n],
            recv_sem=y_rsem.at[yo, n], device_id=twin, device_id_type=MESH,
        ).wait_recv()
        if n < 2:
            hand_over(n, 1, (fin[0, n].astype(F32) + fin[1, n].astype(F32)).astype(BF16))
        else:
            hand_over(yo, 0, fin[yo, 2])
    for k in range(2):
        for h in range(2):
            ref = grads.at[2 * (1 - c) + k, pl.ds(h * half, half), :]
            pltpu.make_async_remote_copy(
                src_ref=ref, dst_ref=ref, send_sem=g_sem.at[0, k, h],
                recv_sem=g_sem.at[1, k, h], device_id=mate, device_id_type=MESH,
            ).wait_recv()
    last = pltpu.make_async_copy(grads, grads_out, out_sem.at[2])
    last.start()
    for copy in waits + hy + hg:
        copy.wait_send()
    for copy in outs + [last]:
        copy.wait()


def solution(mesh):
    F, R = mesh.shape["fsdp"], mesh.shape["rep"]
    X = 2
    Z = F // X
    assert R == 4 and F % X == 0

    def on_device(base, lin, gout, ra, ea, rb, eb):
        T, D = base.shape
        rows, K = ra.shape
        half = rows // 2
        factor = 1.0 / math.sqrt(T * F * R)
        dma = pltpu.SemaphoreType.DMA
        vm = pltpu.VMEM
        any_spec = pl.BlockSpec(memory_space=pl.ANY)
        gli, gbase, grads = pl.pallas_call(
            functools.partial(kernel, F, R),
            out_shape=(
                jax.ShapeDtypeStruct((T, D), BF16),
                jax.ShapeDtypeStruct((T, D), BF16),
                jax.ShapeDtypeStruct((4, rows, K), BF16),
            ),
            in_specs=[any_spec] * 7,
            out_specs=[any_spec] * 3,
            scratch_shapes=[
                vm((T, D), BF16),
                vm((T, D), BF16),
                vm((2, 2, T, D), BF16),
                vm((2, 2, T, K), BF16),
                vm((2, T, D), BF16),
                vm((2, T, K), BF16),
                vm((4, D, K), BF16),
                vm((T, D), F32),
                vm((T, D), BF16),
                vm((T, D), BF16),
                vm((T, D), BF16),
                vm((2, D, K), F32),
                vm((4, rows, K), BF16),
                vm((Z, 2, half, K), BF16),
                vm((Z, 2, half, K), BF16),
                vm((Z, 2, half, K), BF16),
                vm((Z, 2, half, K), BF16),
                vm((Z, half, K), BF16),
                vm((Z, half, K), BF16),
                vm((Z, 3, half, K), BF16),
                vm((2, Z, 3, half, K), BF16),
                vm((3, half, K), F32),
                vm((2, 3, half, K), BF16),
                dma((7,)),
                dma((3,)),
                dma((2, F, 2)),
                dma((2, F, 2)),
                dma((2, F, 2)),
                dma((2, F, 2)),
                dma((2, F, 2)),
                dma((2, F, 2)),
                dma((2, 2)),
                dma((2, 2)),
                dma((2, Z)),
                dma((2, Z)),
                dma((2, Z)),
                dma((Z, 3)),
                dma((2, Z, 3)),
                dma((2, 3)),
                dma((2, 3)),
                dma((2, 2, 2)),
            ],
            compiler_params=pltpu.CompilerParams(
                collective_id=1, has_side_effects=True, vmem_limit_bytes=60 * 1024 * 1024
            ),
        )(base, lin, gout, ra, ea, rb, eb)
        scaled = [grads[w].astype(F32) * factor for w in range(4)]
        return (gli, gbase, *scaled)

    both = P(("fsdp", "rep"), None)
    one = P("fsdp", None)
    return jax.shard_map(
        on_device,
        mesh=mesh,
        in_specs=(both, both, both, one, one, one, one),
        out_specs=(both, both, one, one, one, one),
        check_vma=False,
    )
```

```python
import functools
import math

import jax
import jax.numpy as jnp
from jax import lax
from jax.experimental import pallas as pl
from jax.experimental.pallas import tpu as pltpu
from jax.sharding import PartitionSpec as P

MESH = pl.DeviceIdType.MESH
F32 = jnp.float32
BF16 = jnp.bfloat16


def dot_nn(left, right):
    return lax.dot_general(left, right, (((1,), (0,)), ((), ())), preferred_element_type=F32)


def dot_nt(left, right):
    return lax.dot_general(left, right, (((1,), (1,)), ((), ())), preferred_element_type=F32)


def dot_tn(left, right):
    return lax.dot_general(left, right, (((0,), (0,)), ((), ())), preferred_element_type=F32)


def kernel(
    F,
    R,
    base_in,
    lin_in,
    gout_in,
    ra,
    ea,
    rb,
    eb,
    gli_out,
    gbase_out,
    grads_out,
    base,
    gout,
    own,
    nar,
    peer_wide,
    peer_nar,
    full,
    cross_a,
    gmid,
    gli,
    gbase,
    part,
    grads,
    y1_send,
    y1_recv,
    x1_send,
    x1_recv,
    x2_send,
    x2_recv,
    z_send,
    z_recv,
    last_sum,
    fin,
    load_sem,
    out_sem,
    ag_recv,
    ag_z,
    ag_x,
    ag_y,
    ag_d,
    ag_drecv,
    pw_sem,
    pn_sem,
    y1_sem,
    x1_sem,
    x2_sem,
    zs_sem,
    zr_sem,
    y_ssem,
    y_rsem,
    g_sem,
):
    X = 2
    Z = F // X
    rows = ra.shape[0]
    half = rows // 2
    D = base.shape[1]
    f = lax.axis_index("fsdp")
    r = lax.axis_index("rep")
    z, x = f // X, f % X
    y, c = r // 2, r % 2
    xo = 1 - x
    zp, zm = (z + 1) % Z, (z + Z - 1) % Z

    def dev(ff, rr):
        return {"fsdp": ff, "rep": rr}

    up, down = dev(zp * X + x, r), dev(zm * X + x, r)
    across = dev(z * X + xo, r)
    mate = dev(f, y * 2 + 1 - c)

    twin = dev(f, (1 - y) * 2 + c)

    loads = []
    for i, (src, dst) in enumerate(
        (
            (ra, full.at[0, pl.ds(pl.multiple_of(f * rows, rows), rows), :]),
            (ea, full.at[1, pl.ds(pl.multiple_of(f * rows, rows), rows), :]),
            (rb, full.at[2, pl.ds(pl.multiple_of(f * rows, rows), rows), :]),
            (eb, full.at[3, pl.ds(pl.multiple_of(f * rows, rows), rows), :]),
            (base_in, base),
            (gout_in, gout),
            (lin_in, own.at[0, 0]),
        )
    ):
        copy = pltpu.make_async_copy(src, dst, load_sem.at[i])
        copy.start()
        loads.append(copy)

    barrier = pltpu.get_barrier_semaphore()
    friends = [up, down, across, mate, twin]
    for friend in friends:
        pl.semaphore_signal(barrier, inc=1, device_id=friend, device_id_type=MESH)
    pl.semaphore_wait(barrier, len(friends))
    for copy in loads[:4]:
        copy.wait()

    def push(src, dst, sems, target):
        copy = pltpu.make_async_remote_copy(
            src_ref=src, dst_ref=dst, send_sem=sems[0], recv_sem=sems[1],
            device_id=target, device_id_type=MESH,
        )
        copy.start()
        return copy

    swaps = []

    def swap(src, dst, sem, k):
        swaps.append(push(src.at[1 - c, k], dst.at[k], (sem.at[0, k], sem.at[1, k]), mate))

    sent = []

    def guarded(cond, action):
        if cond is None:
            action()
        else:
            pl.when(cond)(action)

    def also(one, two):
        return one if two is None else two if one is None else jnp.logical_and(one, two)

    def slot(zz, xx):
        return (zz + 2 * Z) % Z * X + xx

    def piece(w, zz, xx, h):
        start = slot(zz, xx) * rows + h * half
        return full.at[w, pl.ds(pl.multiple_of(start, half), half), :]

    def relay(cond, k, zz, xx, h, ssem, rsem, target):
        ref = piece(2 * c + k, zz, xx, h)
        copy = pltpu.make_async_remote_copy(
            src_ref=ref, dst_ref=ref, send_sem=ssem, recv_sem=rsem,
            device_id=target, device_id_type=MESH,
        )
        guarded(cond, copy.start)
        sent.append((cond, copy))

    def zsend(cond, zz, h, upward):
        o = slot(zz, x)
        relay(cond, y, zz, x, h, ag_z.at[upward, o, h], ag_recv.at[y, o, h], up if upward else down)

    def xsend(cond, k, zz, h):
        o = slot(zz, x)
        relay(cond, k, zz, x, h, ag_x.at[k, o, h], ag_recv.at[k, o, h], across)

    def ysend(cond, zz, xx, h):
        o = slot(zz, xx)
        relay(cond, y, zz, xx, h, ag_y.at[y, o, h], ag_recv.at[y, o, h], twin)

    def dsend(cond, k, zz, xx, h):
        o = slot(zz, xx)
        relay(cond, k, zz, xx, h, ag_d.at[k, o, h], ag_drecv.at[k, o, h], mate)

    def arrive(cond, k, zz, xx, h):
        o = slot(zz, xx)
        ref = piece(2 * c + k, zz, xx, h)
        copy = pltpu.make_async_remote_copy(
            src_ref=ref, dst_ref=ref, send_sem=ag_d.at[k, o, h], recv_sem=ag_recv.at[k, o, h],
            device_id=mate, device_id_type=MESH,
        )
        guarded(cond, copy.wait_recv)

    def levels(d):
        if d < 0 or d >= Z:
            return []
        if d == 0:
            return [(z, None, None)]
        return [(z - d, z >= d, True), (z + d, z + d < Z, False)]

    not_top, not_bottom = z < Z - 1, z > 0
    yo = 1 - y

    def stage_line(d):
        for h in range(2):
            for zz, cond, upward in levels(d):
                if d == 0:
                    zsend(not_top, zz, h, 1)
                    zsend(not_bottom, zz, h, 0)
                else:
                    arrive(cond, y, zz, x, h)
                    if d < Z - 1:
                        zsend(also(cond, not_top if upward else not_bottom), zz, h, 1 if upward else 0)
                xsend(cond, y, zz, h)
                if d == 0:
                    if h == 1:
                        xsend(cond, yo, zz, h)
                else:
                    ysend(cond, zz, x, h)
                    dsend(cond, y, zz, x, h)

    def stage_side(d):
        for h in range(2):
            for zz, cond, _ in levels(d):
                arrive(cond, y, zz, xo, h)
                if h == 0:
                    ysend(cond, zz, xo, h)
                dsend(cond, y, zz, xo, h)
                if d > 0:
                    arrive(cond, yo, zz, x, h)
                    if h == 1:
                        xsend(cond, yo, zz, h)
                    dsend(cond, yo, zz, x, h)

    def stage_corner(d):
        for h in range(2):
            for zz, cond, _ in levels(d):
                arrive(cond, yo, zz, xo, h)
                dsend(cond, yo, zz, xo, h)

    stage_line(0)

    for copy in loads[4:]:
        copy.wait()
    tile = min(512, D)

    @pl.loop(0, D // tile)
    def _(t):
        cols = pl.ds(pl.multiple_of(t * tile, tile), tile)
        own[1, 1, :, cols] = (gout[:, cols].astype(F32) * base[:, cols].astype(F32)).astype(BF16)

    swap(own, peer_wide, pw_sem, 1 - c)
    for d in range(1, Z + 2):
        if d < Z:
            stage_line(d)
        stage_side(d - 1)
        stage_corner(d - 2)
    for d in range(Z):
        for zz, cond, _ in levels(d):
            for k in range(2):
                for h in range(2):
                    for near in (True, False):
                        if near and d == 0:
                            continue
                        xx = x if near else xo
                        o = slot(zz, xx)
                        ref = piece(2 * (1 - c) + k, zz, xx, h)
                        copy = pltpu.make_async_remote_copy(
                            src_ref=ref, dst_ref=ref, send_sem=ag_d.at[k, o, h],
                            recv_sem=ag_drecv.at[k, o, h], device_id=mate, device_id_type=MESH,
                        )
                        guarded(cond, copy.wait_recv)
    for cond, copy in sent:
        guarded(cond, copy.wait_send)

    nar[0, 1] = dot_nn(own[0, 0], full[0]).astype(BF16)
    nar[1, 0] = dot_nn(own[1, 1], full[3]).astype(BF16)

    @pl.loop(0, D // tile)
    def _(t):
        cols = pl.ds(pl.multiple_of(t * tile, tile), tile)
        wide = base[:, cols].astype(F32)
        crossed = dot_nt(nar[0, 1], full[1, cols, :])
        cross_a[:, cols] = crossed
        own[1, 0, :, cols] = (own[0, 0, :, cols].astype(F32) + wide * crossed).astype(BF16)
        passed = (gout[:, cols].astype(F32) + dot_nt(nar[1, 0], full[2, cols, :])).astype(BF16)
        gmid[:, cols] = passed
        own[0, 1, :, cols] = (passed.astype(F32) * wide).astype(BF16)

    swap(own, peer_wide, pw_sem, c)
    nar[1, 1] = dot_nn(own[1, 0], full[2]).astype(BF16)
    nar[0, 0] = dot_nn(own[0, 1], full[1]).astype(BF16)

    for k in range(2):
        swap(nar, peer_nar, pn_sem, k)
    for copy in swaps:
        copy.wait()
    level_rows = X * rows

    def products(o):
        cols = pl.ds(pl.multiple_of(o * level_rows, level_rows), level_rows)
        for k in range(2):
            part[k, cols, :] = dot_tn(own[c, k, :, cols], nar[c, k]) + dot_tn(
                peer_wide[k, :, cols], peer_nar[k]
            )

    def mine(k, o, xx, h):
        start = (o * X + xx) * rows + h * half
        return part[k, pl.ds(pl.multiple_of(start, half), half), :]

    flipped = z >= Z // 2
    near_end = jnp.where(flipped, Z - 1 - z, z)

    def owner(i):
        if i == Z - 1:
            return z
        j = Z - 1 - i
        o = jnp.where(j > near_end, j, j - 1)
        return jnp.where(flipped, Z - 1 - o, o)

    sums, waits = [], []

    def first(i):
        o = owner(i)
        products(o)
        for xx in range(2):
            y1_send[o, xx] = mine(yo, o, xx, 0).astype(BF16)
        one = push(y1_send.at[o], y1_recv.at[o], (y1_sem.at[0, o], y1_sem.at[1, o]), twin)
        for k in range(2):
            x1_send[o, k] = mine(k, o, xo, 1).astype(BF16)
        two = push(x1_send.at[o], x1_recv.at[o], (x1_sem.at[0, o], x1_sem.at[1, o]), across)
        waits.extend((one, two))
        sums.append([one, two])

    def second(i):
        o = owner(i)
        one, two = sums[i]
        one.wait_recv()
        x2_send[o] = (mine(y, o, xo, 0) + y1_recv[o, xo].astype(F32)).astype(BF16)
        three = push(x2_send.at[o], x2_recv.at[o], (x2_sem.at[0, o], x2_sem.at[1, o]), across)
        waits.append(three)
        sums[i] = (two, None, three)

    def level_sum(o, n):
        if n == 2:
            return mine(y, o, x, 0) + y1_recv[o, x].astype(F32) + x2_recv[o].astype(F32)
        return mine(n, o, x, 1) + x1_recv[o, n].astype(F32)

    def line(o, n, way, target):
        return pltpu.make_async_remote_copy(
            src_ref=z_send.at[o, n], dst_ref=z_recv.at[way, o, n], send_sem=zs_sem.at[o, n],
            recv_sem=zr_sem.at[way, o, n], device_id=target, device_id_type=MESH,
        )

    def third(i):
        o = owner(i)
        way = jnp.where(o > z, 0, 1)
        target = dev((z + 1 - 2 * way) * X + x, r)
        fed = jnp.where(o > z, z, Z - 1 - z) > 0
        for n in range(3):
            if sums[i][n] is not None:
                sums[i][n].wait_recv()
            value = level_sum(o, n)
            copy = line(o, n, way, target)

            @pl.when(fed)
            def _():
                copy.wait_recv()
                z_send[o, n] = (value + z_recv[way, o, n].astype(F32)).astype(BF16)

            @pl.when(jnp.logical_not(fed))
            def _():
                z_send[o, n] = value.astype(BF16)

            copy.start()
            waits.append(copy)

    def others():
        @pl.loop(0, D // tile)
        def _(t):
            cols = pl.ds(pl.multiple_of(t * tile, tile), tile)
            held = gmid[:, cols].astype(F32)
            crossed = dot_nt(nar[1, 1], full[3, cols, :])
            gbase[:, cols] = (
                gout[:, cols].astype(F32) * crossed + held * cross_a[:, cols]
            ).astype(BF16)
            gli[:, cols] = (held + dot_nt(nar[0, 0], full[0, cols, :])).astype(BF16)

    outs = []
    for i in range(Z - 1):
        first(i)
        if i > 0:
            second(i - 1)
            if i > 1:
                third(i - 2)
    second(Z - 2)
    first(Z - 1)
    others()
    for n, (src, dst) in enumerate(((gli, gli_out), (gbase, gbase_out))):
        copy = pltpu.make_async_copy(src, dst, out_sem.at[n])
        copy.start()
        outs.append(copy)
    second(Z - 1)
    for i in range(max(Z - 3, 0), Z - 1):
        third(i)

    hy = []
    for n in range(3):
        if sums[Z - 1][n] is not None:
            sums[Z - 1][n].wait_recv()
        last_sum[n] = level_sum(z, n)
        for way, cond in ((0, not_bottom), (1, not_top)):

            @pl.when(cond)
            def _():
                line(z, n, way, across).wait_recv()
                last_sum[n] = last_sum[n] + z_recv[way, z, n].astype(F32)

        fin[y, n] = last_sum[n].astype(BF16)
        hy.append(push(fin.at[y, n], fin.at[y, n], (y_ssem.at[y, n], y_rsem.at[y, n]), twin))
    hg = []

    def hand_over(k, h, value):
        grads[2 * c + k, pl.ds(h * half, half), :] = value
        ref = grads.at[2 * c + k, pl.ds(h * half, half), :]
        hg.append(push(ref, ref, (g_sem.at[0, k, h], g_sem.at[1, k, h]), mate))

    hand_over(y, 0, fin[y, 2])
    for n in range(3):
        pltpu.make_async_remote_copy(
            src_ref=fin.at[yo, n], dst_ref=fin.at[yo, n], send_sem=y_ssem.at[yo, n],
            recv_sem=y_rsem.at[yo, n], device_id=twin, device_id_type=MESH,
        ).wait_recv()
        if n < 2:
            hand_over(n, 1, (fin[0, n].astype(F32) + fin[1, n].astype(F32)).astype(BF16))
        else:
            hand_over(yo, 0, fin[yo, 2])
    for k in range(2):
        for h in range(2):
            ref = grads.at[2 * (1 - c) + k, pl.ds(h * half, half), :]
            pltpu.make_async_remote_copy(
                src_ref=ref, dst_ref=ref, send_sem=g_sem.at[0, k, h],
                recv_sem=g_sem.at[1, k, h], device_id=mate, device_id_type=MESH,
            ).wait_recv()
    last = pltpu.make_async_copy(grads, grads_out, out_sem.at[2])
    last.start()
    for copy in waits + hy + hg:
        copy.wait_send()
    for copy in outs + [last]:
        copy.wait()


def solution(mesh):
    F, R = mesh.shape["fsdp"], mesh.shape["rep"]
    X = 2
    Z = F // X
    assert R == 4 and F % X == 0

    def on_device(base, lin, gout, ra, ea, rb, eb):
        T, D = base.shape
        rows, K = ra.shape
        half = rows // 2
        factor = 1.0 / math.sqrt(T * F * R)
        dma = pltpu.SemaphoreType.DMA
        vm = pltpu.VMEM
        any_spec = pl.BlockSpec(memory_space=pl.ANY)
        gli, gbase, grads = pl.pallas_call(
            functools.partial(kernel, F, R),
            out_shape=(
                jax.ShapeDtypeStruct((T, D), BF16),
                jax.ShapeDtypeStruct((T, D), BF16),
                jax.ShapeDtypeStruct((4, rows, K), BF16),
            ),
            in_specs=[any_spec] * 7,
            out_specs=[any_spec] * 3,
            scratch_shapes=[
                vm((T, D), BF16),
                vm((T, D), BF16),
                vm((2, 2, T, D), BF16),
                vm((2, 2, T, K), BF16),
                vm((2, T, D), BF16),
                vm((2, T, K), BF16),
                vm((4, D, K), BF16),
                vm((T, D), F32),
                vm((T, D), BF16),
                vm((T, D), BF16),
                vm((T, D), BF16),
                vm((2, D, K), F32),
                vm((4, rows, K), BF16),
                vm((Z, 2, half, K), BF16),
                vm((Z, 2, half, K), BF16),
                vm((Z, 2, half, K), BF16),
                vm((Z, 2, half, K), BF16),
                vm((Z, half, K), BF16),
                vm((Z, half, K), BF16),
                vm((Z, 3, half, K), BF16),
                vm((2, Z, 3, half, K), BF16),
                vm((3, half, K), F32),
                vm((2, 3, half, K), BF16),
                dma((7,)),
                dma((3,)),
                dma((2, F, 2)),
                dma((2, F, 2)),
                dma((2, F, 2)),
                dma((2, F, 2)),
                dma((2, F, 2)),
                dma((2, F, 2)),
                dma((2, 2)),
                dma((2, 2)),
                dma((2, Z)),
                dma((2, Z)),
                dma((2, Z)),
                dma((Z, 3)),
                dma((2, Z, 3)),
                dma((2, 3)),
                dma((2, 3)),
                dma((2, 2, 2)),
            ],
            compiler_params=pltpu.CompilerParams(
                collective_id=1, has_side_effects=True, vmem_limit_bytes=60 * 1024 * 1024
            ),
        )(base, lin, gout, ra, ea, rb, eb)
        scaled = [grads[w].astype(F32) * factor for w in range(4)]
        return (gli, gbase, *scaled)

    both = P(("fsdp", "rep"), None)
    one = P("fsdp", None)
    return jax.shard_map(
        on_device,
        mesh=mesh,
        in_specs=(both, both, both, one, one, one, one),
        out_specs=(both, both, one, one, one, one),
        check_vma=False,
    )
```
